128 devices in a mesh: isl: 4 (over z_hi, core), fsdp: 32 (over x, z_lo, y).
Axes of the slice: x: 4, y: 4, z: 4 (z_hi: 2, z_lo: 2; z = z_hi * 2 + z_lo), core: 2. Of those that a mesh axis runs over, the one named last changes fastest.
Arguments:
- weights: float32 [3, 7168, 4096], P(None, 'fsdp', 'isl'), may hold values from -6 to 6
- momentum: float32 [3, 7168, 4096], P(None, 'fsdp', 'isl'), may hold values from -0.12 to 0.12
- first_moment: bfloat16 [4, 3, 7168, 4096], P('isl', None, 'fsdp'), may hold values from -0.00029945374 to 0.00029945374
- second_moment: bfloat16 [4, 3, 7168, 4096], P('isl', None, 'fsdp'), may hold values from 9.95351e-09 to 9.953976e-06
- inputs: bfloat16 [2, 1024, 4096], P(None, ('isl', 'fsdp')), may hold values from -6 to 6
- targets: bfloat16 [2, 1024, 4096], P(None, ('isl', 'fsdp')), may hold values from -6 to 6
- overflow_step: int32 [4, 32], P('isl', 'fsdp'), may hold values from 0 to 63
Outputs:
- new_weights: float32 [3, 7168, 4096], P(None, 'fsdp', 'isl')
- new_momentum: float32 [3, 7168, 4096], P(None, 'fsdp', 'isl')
The draws below stay inside these ranges and needn't reach their ends.
Inputs may be any that keep to these rules, and one draw needn't show every extreme that they name: `overflow_step`: A device reports an overflow at inner step k when its value equals k; values of 2 or more report none.
All inputs are finite; a program needn't handle non-finite values.
Results may differ from the reference program's by a relative error of at most 0.004.
Values may be sent and summed in bfloat16 or wider, within the bound.
No kernel may reach another device: no remote copies, remote signals or barrier semaphores. Data moves between devices by JAX's collectives and lax.ppermute only.
A program may use at most 128 MiB of HBM per device.

```python
import math
import jax
import jax.numpy as jnp
from jax import lax

D = 4096
FF = 7168
TOK_DEV = 8
INNER = 2
TOKENS = 1024
N_ISL = 4
N_FSDP = 32


def set_ends(drawn, key, least, high):
    longest = drawn.shape.index(max(drawn.shape))
    spots = []
    for shift in (0, 1):
        where = [jax.random.randint(jax.random.fold_in(key, axis), (), 0, length) for axis, length in enumerate(drawn.shape)]
        where[longest] = (where[longest] + shift) % drawn.shape[longest]
        spots.append(tuple(where))
    return drawn.at[spots[0]].set(least).at[spots[1]].set(high)


def block_scale(rng, extent, pieces, low, largest):
    factor_of, own = 1.0, jax.random.fold_in(rng, 6)
    for position, blocks in pieces:
        heights = jnp.exp(jax.random.uniform(jax.random.fold_in(own, position), (blocks,), jnp.float32, low / len(pieces), largest / len(pieces)))
        factor_of = factor_of * jnp.repeat(heights, extent[position] // blocks).reshape([-1 if axis == position else 1 for axis in range(len(extent))])
    return factor_of


def bell_draw(stream_key, dims, deviation, reach, pieces=(), held_as=jnp.bfloat16):
    drawn = deviation * jax.random.normal(stream_key, dims, jnp.float32)
    if pieces:
        drawn = drawn * block_scale(stream_key, dims, pieces, -0.22, 0.18)
    return jnp.clip(drawn, -reach, reach).astype(held_as)


def setup_inputs(seed: int = 0) -> dict:
    key_of = jax.random.split(jax.random.key(seed), 8)
    weights = bell_draw(key_of[0], (3, FF, D), 1.0, 6.0, ((1, 32), (2, 4)), jnp.float32)
    momentum = bell_draw(key_of[1], (3, FF, D), 0.02, 0.12, ((1, 32), (2, 4)), jnp.float32)
    first_moment = bell_draw(key_of[2], (N_ISL, 3, FF, D), 0.00005, 0.00029945374, ((0, 4), (2, 32)))
    second_moment = jnp.clip(jnp.exp(math.log(9.953975677490234e-06) - 6.907802 * jax.random.uniform(key_of[3], (N_ISL, 3, FF, D), jnp.float32) ** block_scale(key_of[3], (N_ISL, 3, FF, D), ((0, 4), (2, 32)), -0.2, 0.2)), 9.953510016202927e-09, 9.953975677490234e-06).astype(jnp.bfloat16)
    inputs = bell_draw(key_of[4], (INNER, TOKENS, D), 1.0, 6.0, ((1, 128),))
    targets = bell_draw(key_of[5], (INNER, TOKENS, D), 1.0, 6.0, ((1, 128),))
    overflow_step = set_ends(jax.random.randint(key_of[6], (N_ISL, N_FSDP), 0, 2 * N_FSDP), jax.random.fold_in(key_of[6], 1), 0, (2 * N_FSDP) - 1).astype(jnp.int32)
    return {"weights": weights, "momentum": momentum, "first_moment": first_moment, "second_moment": second_moment, "inputs": inputs, "targets": targets, "overflow_step": overflow_step}


inner_rate = 0.02
beta_first = 0.9
beta_second = 0.95
epsilon = 1e-08
decay_rate = 0.1
outer_rate = 0.7
nesterov_coef = 0.9

def silu_parts(preact):
    sigmoid_value = jax.nn.sigmoid(preact)
    return (preact * sigmoid_value, sigmoid_value * (1.0 + preact * (1.0 - sigmoid_value)))

def island_gradient(rounded, block_inputs, block_targets):
    token_count = block_inputs.shape[0]
    gate_pre = jnp.dot(block_inputs, rounded[0].T, preferred_element_type=jnp.float32) / math.sqrt(D)
    up_pre = jnp.dot(block_inputs, rounded[1].T, preferred_element_type=jnp.float32) / math.sqrt(D)
    activated, slope = silu_parts(gate_pre)
    hidden = (activated * up_pre).astype(jnp.bfloat16)
    summed = jnp.dot(hidden, rounded[2], preferred_element_type=jnp.float32)
    outputs = block_inputs.astype(jnp.float32) + summed / math.sqrt(FF)
    slopes = ((outputs - block_targets.astype(jnp.float32)) / token_count).astype(jnp.bfloat16)
    hidden_slope = jnp.dot(slopes, rounded[2].T, preferred_element_type=jnp.float32) / math.sqrt(FF)
    gate_slope = (hidden_slope * up_pre * slope).astype(jnp.bfloat16)
    up_slope = (hidden_slope * activated).astype(jnp.bfloat16)
    grad_gate = jnp.dot(gate_slope.T, block_inputs, preferred_element_type=jnp.float32) / math.sqrt(D)
    grad_up = jnp.dot(up_slope.T, block_inputs, preferred_element_type=jnp.float32) / math.sqrt(D)
    grad_down = jnp.dot(hidden.T, slopes, preferred_element_type=jnp.float32) / math.sqrt(FF)
    return jnp.stack([grad_gate, grad_up, grad_down])

def reference(weights, momentum, first_moment, second_moment, inputs, targets, overflow_step):
    island_tokens = TOK_DEV * N_FSDP
    pseudo_sum = jnp.zeros(weights.shape, jnp.float32)
    for island in range(N_ISL):
        current = weights
        moment_one = first_moment[island].astype(jnp.float32)
        moment_two = second_moment[island].astype(jnp.float32)
        for inner_step in range(INNER):
            begin = island * island_tokens
            block_inputs = inputs[inner_step, begin:begin + island_tokens]
            block_targets = targets[inner_step, begin:begin + island_tokens]
            gradient = island_gradient(current.astype(jnp.bfloat16), block_inputs, block_targets)
            overflow_count = jnp.sum((overflow_step[island] == inner_step).astype(jnp.int32))
            skipped = overflow_count > 0
            next_one = beta_first * moment_one + (1.0 - beta_first) * gradient
            next_two = beta_second * moment_two + (1.0 - beta_second) * gradient * gradient
            next_weights = current - inner_rate * (next_one / (jnp.sqrt(next_two) + epsilon) + decay_rate * current)
            current = jnp.where(skipped, current, next_weights)
            moment_one = jnp.where(skipped, moment_one, next_one)
            moment_two = jnp.where(skipped, moment_two, next_two)
        pseudo = (weights - current).astype(jnp.bfloat16)
        pseudo_sum = pseudo_sum + lax.optimization_barrier(pseudo).astype(jnp.float32)
    outer_delta = pseudo_sum / N_ISL
    new_momentum = nesterov_coef * momentum + outer_delta
    new_weights = weights - outer_rate * (outer_delta + nesterov_coef * new_momentum)
    return (new_weights, new_momentum)
```

```python
import functools
import math

import jax
import jax.numpy as jnp
from jax import lax
from jax.experimental import pallas as pl
from jax.experimental.pallas import tpu as pltpu
from jax.sharding import Mesh
from jax.sharding import PartitionSpec as P


D = 4096
FF = 7168

inner_rate = 0.02
beta_first = 0.9
beta_second = 0.95
epsilon = 1e-08
decay_rate = 0.1
outer_rate = 0.7
nesterov_coef = 0.9


bf16, f32 = jnp.bfloat16, jnp.float32

FSDP = ("x", "y", "zl")
SIZES = {"x": 4, "y": 4, "zl": 2}


def around(own, dim):
    n = SIZES[dim]
    return [own] + [lax.ppermute(own, dim, [(i, (i - s) % n) for i in range(n)]) for s in range(1, n)]


def collect(own, dim):
    n = SIZES[dim]
    blocks = around(own, dim)
    ring = jnp.stack(blocks + blocks[:-1])
    return lax.dynamic_slice_in_dim(ring, (n - lax.axis_index(dim)) % n, n, axis=0)


def contract_last(left, right):
    return lax.dot_general(left, right, (((1,), (1,)), ((), ())), preferred_element_type=f32)


VM = pl.BlockSpec(memory_space=pltpu.VMEM)
SM = pl.BlockSpec(memory_space=pltpu.SMEM)
MIB = 1 << 20


def forward_kernel(n_w, at_ref, *refs):
    pieces, refs = refs[:8], refs[8:]
    w_refs, refs = refs[:n_w], refs[n_w:]
    x_out, gate_out, up_out, hidden_out, p_out = refs[:5]
    turn = refs[-1]
    quarter = x_out.shape[1] // 4
    half = 2 * quarter

    def w(p, r):
        if n_w == 1:
            return w_refs[0][p, r]
        return w_refs[2 * r][p] if p < 2 else w_refs[2 * r + 1][0]

    plane = pieces[0].shape[0]
    block = plane // 4
    for s in range(4):
        row = pl.multiple_of(((at_ref[0] + s) % 4) * plane, plane)
        x_out[pl.ds(row, plane), 0:half] = pieces[s][...]
        for x in range(4):
            row = pl.multiple_of(x * plane + ((at_ref[1] + s) % 4) * block, block)
            x_out[pl.ds(row, block), half:] = pieces[4 + s][x * block : (x + 1) * block, 0:half]
    if n_w > 1:
        for p in range(3):
            for r in range(4):
                refs[5][p, r] = w(p, r)
    gate, up = None, None
    for r in range(4):
        x = x_out[:, r * quarter : (r + 1) * quarter]
        g, u = contract_last(w(0, r), x), contract_last(w(1, r), x)
        gate = g if gate is None else gate + g
        up = u if up is None else up + u
    gate = gate * (1.0 / math.sqrt(D))
    up = up * (1.0 / math.sqrt(D))
    gate_out[...] = gate
    up_out[...] = up
    hidden = (gate * jax.nn.sigmoid(gate)) * up
    hidden_out[...] = hidden.astype(bf16)
    rows = hidden.shape[0]
    turn[...] = jnp.zeros_like(turn)
    turn[0:rows, :] = hidden
    turned = turn[...].T[:, 0:rows].astype(bf16)
    for r in range(4):
        part = jnp.dot(turned, w(2, r), preferred_element_type=f32)
        p_out[:, r * quarter : (r + 1) * quarter] = part.astype(bf16)


def forward(at, pieces, w, rows):
    first = isinstance(w, list)
    tokens, width = 4 * pieces[0].shape[0], 2 * pieces[0].shape[1]
    square = -(-max(rows, tokens) // 128) * 128
    small = jax.ShapeDtypeStruct((rows, tokens), f32)
    wide = jax.ShapeDtypeStruct((tokens, width), bf16)
    outs = [wide, small, small, jax.ShapeDtypeStruct((rows, tokens), bf16), wide]
    if first:
        outs.append(jax.ShapeDtypeStruct((3, 4, rows, width // 4), bf16))
    weights = w if first else [w]
    return pl.pallas_call(
        functools.partial(forward_kernel, len(weights)),
        out_shape=outs,
        in_specs=[SM] + [VM] * (8 + len(weights)),
        out_specs=[VM] * len(outs),
        scratch_shapes=[pltpu.VMEM((square, tokens), f32)],
        compiler_params=pltpu.CompilerParams(vmem_limit_bytes=24 * MIB),
        cost_estimate=pl.CostEstimate(flops=6 * rows * tokens * width, bytes_accessed=8 << 20, transcendentals=0),
        name="forward0" if first else "forward1",
    )(at, *pieces, *weights)


def slopes_kernel(scale, parts_ref, x_ref, y_ref, out_ref):
    width = x_ref.shape[1]
    lanes = min(512, width)
    for low in range(0, width, lanes):
        cols = slice(low, low + lanes)
        total = parts_ref[0, :, cols].astype(f32)
        for k in range(1, parts_ref.shape[0]):
            total = total + parts_ref[k, :, cols].astype(f32)
        outputs = x_ref[:, cols].astype(f32) + total * (1.0 / math.sqrt(FF))
        slopes = ((outputs - y_ref[:, cols].astype(f32)) * scale).astype(bf16)
        for k in range(out_ref.shape[0]):
            out_ref[k, :, cols] = slopes


def own_slopes(parts, x, y):
    n, tok, width = parts.shape
    return pl.pallas_call(
        functools.partial(slopes_kernel, 1.0 / (n * tok)),
        out_shape=jax.ShapeDtypeStruct(parts.shape, bf16),
        in_specs=[VM, VM, VM],
        out_specs=VM,
        compiler_params=pltpu.CompilerParams(vmem_limit_bytes=8 * MIB),
        cost_estimate=pl.CostEstimate(flops=n * tok * width, bytes_accessed=4 * n * tok * width, transcendentals=0),
        name="own_slopes",
    )(parts, x, y)


def slope_kernel(z_ref, w_ref, gate_ref, up_ref, hidden_ref, s_out):
    quarter = w_ref.shape[-1]
    slope = None
    for r in range(4):
        part = contract_last(w_ref[2, r], z_ref[:, r * quarter : (r + 1) * quarter])
        slope = part if slope is None else slope + part
    slope = slope * (1.0 / math.sqrt(FF))
    gate = gate_ref[...]
    sig = jax.nn.sigmoid(gate)
    s_out[0] = (slope * up_ref[...] * (sig * (1.0 + gate * (1.0 - sig)))).astype(bf16)
    s_out[1] = (slope * (gate * sig)).astype(bf16)
    s_out[2] = hidden_ref[...]


def slope_parts(z, w, gate, up, hidden):
    rows, tokens = gate.shape
    width = z.shape[1]
    return pl.pallas_call(
        slope_kernel,
        out_shape=jax.ShapeDtypeStruct((3, rows, tokens), bf16),
        in_specs=[VM] * 5,
        out_specs=VM,
        compiler_params=pltpu.CompilerParams(vmem_limit_bytes=12 * MIB),
        cost_estimate=pl.CostEstimate(flops=2 * rows * tokens * width, bytes_accessed=4 << 20, transcendentals=0),
        name="slope_parts",
    )(z, w, gate, up, hidden)


def adam_step(m, v, c, g, k):
    m = k[0] * m + k[1] * g
    v = k[2] * v + k[3] * (g * g)
    root = v * lax.rsqrt(v)
    c = k[4] * c - k[5] * (m / (root + epsilon))
    return m, v, c


def adam_kernel(steps, ps, r_of, lanes, pos, coef, m_ref, v_ref, w_ref, *refs):
    ins = [refs[3 * s : 3 * s + 3] for s in range(steps)]
    out_ref = refs[3 * steps]
    g_refs = refs[3 * steps + 1 :]
    i = pl.program_id(0)
    r = r_of(i)
    _, rows, quarter = g_refs[0].shape
    across = pl.ds(pl.multiple_of(r * quarter, quarter), quarter)
    for n, p in enumerate(ps):
        for s in range(steps):
            x_ref, z_ref, s_ref = ins[s]
            right = (x_ref if p < 2 else z_ref)[:, across]
            g_refs[s][n] = jnp.dot(s_ref[p], right, preferred_element_type=f32)
    step_rows = 16
    for n, p in enumerate(ps):
        ks = [[coef[12 * s + (6 if p == 2 else 0) + j] for j in range(6)] for s in range(steps)]

        @pl.loop(0, rows // step_rows, unroll=2 if (rows // step_rows) % 2 == 0 else 1)
        def _(k, n=n, p=p, ks=ks):
            at = pl.ds(pl.multiple_of(k * step_rows, step_rows), step_rows)
            for low in range(0, quarter, lanes):
                cols = slice(low, low + lanes)
                m = m_ref[0, n, at, cols].astype(f32)
                v = v_ref[0, n, at, cols].astype(f32)
                start = w_ref[p, r, at, cols].astype(f32)
                c = start
                for s in range(steps):
                    m, v, c = adam_step(m, v, c, g_refs[s][n, at, cols], ks[s])
                out_ref[n, i, at, cols] = (c if steps == 1 else start - c).astype(bf16)


def adam(pos, coef, first_moment, second_moment, w, parts, tiles):
    ps, rs = list(tiles[0]), list(tiles[1])
    steps = len(parts)
    rows, quarter = w.shape[2:]
    tokens = parts[0][0].shape[0]
    np_, nr = len(ps), len(rs)
    stride = rs[1] - rs[0] if nr > 1 else 0
    assert rs == [rs[0] + stride * k for k in range(nr)] and ps == list(range(ps[0], ps[0] + np_)) and ps[0] % np_ == 0

    def r_of(i):
        return rs[0] + stride * i

    moment = pl.BlockSpec((1, np_, rows, quarter), lambda i, pos: (0, ps[0] // np_, 0, r_of(i) ^ pos[0]))
    args = [a for part in parts for a in part]
    return pl.pallas_call(
        functools.partial(adam_kernel, steps, ps, r_of, min(512, quarter)),
        out_shape=jax.ShapeDtypeStruct((np_, nr, rows, quarter), bf16),
        grid_spec=pltpu.PrefetchScalarGridSpec(
            num_scalar_prefetch=1,
            grid=(nr,),
            in_specs=[SM, moment, moment, VM] + [VM] * (3 * steps),
            out_specs=VM,
            scratch_shapes=[pltpu.VMEM((np_, rows, quarter), f32)] * steps,
        ),
        compiler_params=pltpu.CompilerParams(vmem_limit_bytes=32 * MIB),
        cost_estimate=pl.CostEstimate(
            flops=np_ * nr * steps * 2 * rows * tokens * quarter, bytes_accessed=np_ * nr * rows * quarter * 8, transcendentals=0
        ),
    )(pos, coef, first_moment, second_moment, w, *args)


def coefficients(skipped):
    found = []
    for s in range(2):
        for scale in (1.0 / math.sqrt(D), 1.0 / math.sqrt(FF)):
            go = (beta_first, (1.0 - beta_first) * scale, beta_second, (1.0 - beta_second) * scale * scale, 1.0 - inner_rate * decay_rate, inner_rate)
            stay = (1.0, 0.0, 1.0, 0.0, 1.0, 0.0)
            found.append(jnp.where(skipped[s], jnp.array(stay, f32), jnp.array(go, f32)))
    return jnp.concatenate(found)


def round_of(weights, momentum, first_moment, second_moment, inputs, targets, overflow_step):
    _, rows, quarter = weights.shape
    zh, co = lax.axis_index("zh"), lax.axis_index("co")
    mine = 2 * zh + co

    def own_order(array):
        parts = [lax.dynamic_slice_in_dim(array, (mine ^ r) * quarter, quarter, axis=2) for r in range(4)]
        return jnp.concatenate(parts, axis=2)

    def partner(array):
        return lax.ppermute(array, "co", [(0, 1), (1, 0)])

    def across(array):
        return lax.ppermute(array, "zh", [(0, 1), (1, 0)])

    own = [weights[0:2].astype(bf16), weights[2:3].astype(bf16)]
    far = [across(chunk) for chunk in own]
    near = [partner(chunk) for chunk in own]
    both = [partner(chunk) for chunk in far]
    w = own + near + far + both

    inputs, targets = own_order(inputs), own_order(targets)
    steps, tok, width = inputs.shape
    half = width // 2
    marks = (overflow_step.reshape(1, 1) == jnp.arange(128, dtype=jnp.int32).reshape(1, 128)).astype(bf16)
    marks = jnp.broadcast_to(marks, (tok, 128))
    pair = collect(jnp.concatenate([inputs[0], marks, inputs[1]], axis=1), "zl")
    pieces = []
    for k in range(steps):
        low = k * (width + 128)
        first, second = pair[..., low : low + half], pair[..., low + half : low + width + (128 if k == 0 else 0)]
        if k:
            first, second, *middle = lax.optimization_barrier((first, second, *middle))
        middle = [collect(first, "y"), collect(second, "x")]
        flat = [m.reshape(-1, m.shape[-1]) for m in middle]
        pieces.append(around(flat[0], "x") + around(flat[1], "y"))
    marked = functools.reduce(jnp.maximum, [jnp.max(p[:, half : half + steps], axis=0) for p in pieces[0][4:]])
    coef = coefficients([marked[s] > 0 for s in range(steps)])
    pos = mine.reshape(1).astype(jnp.int32)
    at = jnp.stack([lax.axis_index("x"), lax.axis_index("y")]).astype(jnp.int32)

    parts = []
    w_start = None
    for k in range(steps):
        x, gate, up, hidden, sums, *w0 = forward(at, pieces[k], w, rows)
        if k == 0:
            w = w_start = w0[0]
        arrived = lax.all_to_all(sums.reshape(-1, tok, width), FSDP, 0, 0, tiled=True)
        copies = own_slopes(arrived, inputs[k], targets[k])
        z = lax.all_to_all(copies, FSDP, 0, 0, tiled=True).reshape(-1, width)
        parts.append((x, z, slope_parts(z, w, gate, up, hidden)))
        if k == 0:
            w = adam(pos, coef, first_moment, second_moment, w, parts, (range(3), range(4)))
    arrived = []
    for p in (2, 0, 1):
        pair = adam(pos, coef, first_moment, second_moment, w_start, parts, ((p,), (3, 2)))
        joint = (pair[0, 1].astype(f32) + partner(pair[0, 0]).astype(f32)).astype(bf16)
        joint, pos = lax.optimization_barrier((joint, pos))
        arrived.append((p, across(joint)))
    rest = adam(pos, coef, first_moment, second_moment, w_start, parts, (range(3), (1, 0)))
    near_part = partner(rest[:, 0])
    arrived = jnp.stack([a for _, a in sorted(arrived, key=lambda e: e[0])])
    delta = (rest[:, 1].astype(f32) + near_part.astype(f32) + arrived.astype(f32)) / 4
    new_momentum = nesterov_coef * momentum + delta
    new_weights = weights - outer_rate * (delta + nesterov_coef * new_momentum)
    return (new_weights, new_momentum)


def solution(mesh):
    grid = Mesh(mesh.devices.reshape(2, 2, 4, 2, 4), ("zh", "co", "x", "zl", "y"))
    isl, fsdp = ("zh", "co"), ("x", "zl", "y")
    in_specs = (
        P(None, fsdp, isl),
        P(None, fsdp, isl),
        P(isl, None, fsdp, None),
        P(isl, None, fsdp, None),
        P(None, isl + fsdp, None),
        P(None, isl + fsdp, None),
        P(isl, fsdp),
    )
    out_specs = (P(None, fsdp, isl), P(None, fsdp, isl))
    return jax.shard_map(round_of, mesh=grid, in_specs=in_specs, out_specs=out_specs, check_vma=False)
```

```python
import functools
import math

import jax
import jax.numpy as jnp
from jax import lax
from jax.experimental import pallas as pl
from jax.experimental.pallas import tpu as pltpu
from jax.sharding import Mesh
from jax.sharding import PartitionSpec as P


D = 4096
FF = 7168

inner_rate = 0.02
beta_first = 0.9
beta_second = 0.95
epsilon = 1e-08
decay_rate = 0.1
outer_rate = 0.7
nesterov_coef = 0.9


bf16, f32 = jnp.bfloat16, jnp.float32

FSDP = ("x", "y", "zl")
SIZES = {"x": 4, "y": 4, "zl": 2}


def around(own, dim):
    n = SIZES[dim]
    return [own] + [lax.ppermute(own, dim, [(i, (i - s) % n) for i in range(n)]) for s in range(1, n)]


def collect(own, dim):
    n = SIZES[dim]
    blocks = around(own, dim)
    ring = jnp.stack(blocks + blocks[:-1])
    return lax.dynamic_slice_in_dim(ring, (n - lax.axis_index(dim)) % n, n, axis=0)


def contract_last(left, right):
    return lax.dot_general(left, right, (((1,), (1,)), ((), ())), preferred_element_type=f32)


VM = pl.BlockSpec(memory_space=pltpu.VMEM)
SM = pl.BlockSpec(memory_space=pltpu.SMEM)
MIB = 1 << 20
FORWARD_MIB, ADAM_MIB, SMALL_MIB = 6, 13, 4


def forward_kernel(step, n_w, at_ref, *refs):
    pieces, refs = refs[:8], refs[8:]
    w_refs, refs = refs[:n_w], refs[n_w:]
    x_out, gate_out, up_out, hidden_out, p_out = refs[:5]
    turn = refs[-1]
    quarter = x_out.shape[1] // 4
    half = 2 * quarter

    def w(p, r):
        if n_w == 1:
            return w_refs[0][p, r]
        return w_refs[2 * r][p] if p < 2 else w_refs[2 * r + 1][0]

    plane = pieces[0].shape[0]
    block = plane // 4
    cols = slice(step * half, (step + 1) * half)
    for s in range(4):
        row = pl.multiple_of(((at_ref[0] + s) % 4) * plane, plane)
        x_out[pl.ds(row, plane), 0:half] = pieces[s][:, cols]
        for x in range(4):
            row = pl.multiple_of(x * plane + ((at_ref[1] + s) % 4) * block, block)
            x_out[pl.ds(row, block), half:] = pieces[4 + s][x * block : (x + 1) * block, cols]
    if n_w > 1:
        for p in range(3):
            for r in range(4):
                refs[5][p, r] = w(p, r)
    gate, up = None, None
    for r in range(4):
        x = x_out[:, r * quarter : (r + 1) * quarter]
        g, u = contract_last(w(0, r), x), contract_last(w(1, r), x)
        gate = g if gate is None else gate + g
        up = u if up is None else up + u
    gate = gate * (1.0 / math.sqrt(D))
    up = up * (1.0 / math.sqrt(D))
    gate_out[...] = gate
    up_out[...] = up
    hidden = (gate * jax.nn.sigmoid(gate)) * up
    hidden_out[...] = hidden.astype(bf16)
    rows = hidden.shape[0]
    turn[...] = jnp.zeros_like(turn)
    turn[0:rows, :] = hidden
    turned = turn[...].T[:, 0:rows].astype(bf16)
    for r in range(4):
        part = jnp.dot(turned, w(2, r), preferred_element_type=f32)
        p_out[:, r * quarter : (r + 1) * quarter] = part.astype(bf16)


def forward(at, step, pieces, w, rows):
    first = isinstance(w, list)
    tokens, width = 4 * pieces[0].shape[0], pieces[0].shape[1]
    square = -(-max(rows, tokens) // 128) * 128
    small = pltpu.VMEM((rows, tokens), f32)
    wide = jax.ShapeDtypeStruct((tokens, width), bf16)
    outs = [pltpu.VMEM((tokens, width), bf16), small, small, pltpu.VMEM((rows, tokens), bf16), wide]
    if first:
        outs.append(pltpu.VMEM((3, 4, rows, width // 4), bf16))
    weights = w if first else [w]
    return pl.pallas_call(
        functools.partial(forward_kernel, step, len(weights)),
        out_shape=outs,
        in_specs=[SM] + [VM] * (8 + len(weights)),
        out_specs=[VM] * len(outs),
        scratch_shapes=[pltpu.VMEM((square, tokens), f32)],
        compiler_params=pltpu.CompilerParams(vmem_limit_bytes=FORWARD_MIB * MIB),
        cost_estimate=pl.CostEstimate(flops=6 * rows * tokens * width, bytes_accessed=8 << 20, transcendentals=0),
        name="forward0" if first else "forward1",
    )(at, *pieces, *weights)


def slopes_kernel(scale, parts_ref, x_ref, y_ref, out_ref):
    width = x_ref.shape[1]
    lanes = min(512, width)
    for low in range(0, width, lanes):
        cols = slice(low, low + lanes)
        total = parts_ref[0, :, cols].astype(f32)
        for k in range(1, parts_ref.shape[0]):
            total = total + parts_ref[k, :, cols].astype(f32)
        outputs = x_ref[:, cols].astype(f32) + total * (1.0 / math.sqrt(FF))
        slopes = ((outputs - y_ref[:, cols].astype(f32)) * scale).astype(bf16)
        for k in range(out_ref.shape[0]):
            out_ref[k, :, cols] = slopes


def own_slopes(parts, x, y):
    n, tok, width = parts.shape
    return pl.pallas_call(
        functools.partial(slopes_kernel, 1.0 / (n * tok)),
        out_shape=jax.ShapeDtypeStruct(parts.shape, bf16),
        in_specs=[VM, VM, VM],
        out_specs=VM,
        compiler_params=pltpu.CompilerParams(vmem_limit_bytes=SMALL_MIB * MIB),
        cost_estimate=pl.CostEstimate(flops=n * tok * width, bytes_accessed=4 * n * tok * width, transcendentals=0),
        name="own_slopes",
    )(parts, x, y)


def slope_kernel(z_ref, w_ref, gate_ref, up_ref, hidden_ref, s_out):
    quarter = w_ref.shape[-1]
    slope = None
    for r in range(4):
        part = contract_last(w_ref[2, r], z_ref[:, r * quarter : (r + 1) * quarter])
        slope = part if slope is None else slope + part
    slope = slope * (1.0 / math.sqrt(FF))
    gate = gate_ref[...]
    sig = jax.nn.sigmoid(gate)
    s_out[0] = (slope * up_ref[...] * (sig * (1.0 + gate * (1.0 - sig)))).astype(bf16)
    s_out[1] = (slope * (gate * sig)).astype(bf16)
    s_out[2] = hidden_ref[...]


def slope_parts(z, w, gate, up, hidden):
    rows, tokens = gate.shape
    width = z.shape[1]
    return pl.pallas_call(
        slope_kernel,
        out_shape=pltpu.VMEM((3, rows, tokens), bf16),
        in_specs=[VM] * 5,
        out_specs=VM,
        compiler_params=pltpu.CompilerParams(vmem_limit_bytes=SMALL_MIB * MIB),
        cost_estimate=pl.CostEstimate(flops=2 * rows * tokens * width, bytes_accessed=4 << 20, transcendentals=0),
        name="slope_parts",
    )(z, w, gate, up, hidden)


def adam_step(m, v, c, g, k):
    m = k[0] * m + k[1] * g
    v = k[2] * v + k[3] * (g * g)
    root = v * lax.rsqrt(v)
    c = k[4] * c - k[5] * (m / (root + epsilon))
    return m, v, c


def adam_kernel(steps, ps, r_of, lanes, pos, coef, m_ref, v_ref, w_ref, *refs):
    ins = [refs[3 * s : 3 * s + 3] for s in range(steps)]
    out_ref = refs[3 * steps]
    g_refs = refs[3 * steps + 1 :]
    i = pl.program_id(0)
    r = r_of(i)
    _, rows, quarter = g_refs[0].shape
    across = pl.ds(pl.multiple_of(r * quarter, quarter), quarter)
    for n, p in enumerate(ps):
        for s in range(steps):
            x_ref, z_ref, s_ref = ins[s]
            right = (x_ref if p < 2 else z_ref)[:, across]
            g_refs[s][n] = jnp.dot(s_ref[p], right, preferred_element_type=f32)
    step_rows = 16
    for n, p in enumerate(ps):
        ks = [[coef[12 * s + (6 if p == 2 else 0) + j] for j in range(6)] for s in range(steps)]

        @pl.loop(0, rows // step_rows, unroll=2 if (rows // step_rows) % 2 == 0 else 1)
        def _(k, n=n, p=p, ks=ks):
            at = pl.ds(pl.multiple_of(k * step_rows, step_rows), step_rows)
            for low in range(0, quarter, lanes):
                cols = slice(low, low + lanes)
                m = m_ref[0, n, at, cols].astype(f32)
                v = v_ref[0, n, at, cols].astype(f32)
                start = w_ref[p, r, at, cols].astype(f32)
                c = start
                for s in range(steps):
                    m, v, c = adam_step(m, v, c, g_refs[s][n, at, cols], ks[s])
                out_ref[n, i, at, cols] = (c if steps == 1 else start - c).astype(bf16)


def adam(pos, coef, first_moment, second_moment, w, parts, tiles):
    ps, rs = list(tiles[0]), list(tiles[1])
    steps = len(parts)
    rows, quarter = w.shape[2:]
    tokens = parts[0][0].shape[0]
    np_, nr = len(ps), len(rs)
    stride = rs[1] - rs[0] if nr > 1 else 0
    assert rs == [rs[0] + stride * k for k in range(nr)] and ps == list(range(ps[0], ps[0] + np_)) and ps[0] % np_ == 0

    def r_of(i):
        return rs[0] + stride * i

    moment = pl.BlockSpec((1, np_, rows, quarter), lambda i, pos: (0, ps[0] // np_, 0, r_of(i) ^ pos[0]))
    args = [a for part in parts for a in part]
    return pl.pallas_call(
        functools.partial(adam_kernel, steps, ps, r_of, min(512, quarter)),
        out_shape=pltpu.VMEM((np_, nr, rows, quarter), bf16),
        grid_spec=pltpu.PrefetchScalarGridSpec(
            num_scalar_prefetch=1,
            grid=(nr,),
            in_specs=[SM, moment, moment, VM] + [VM] * (3 * steps),
            out_specs=VM,
            scratch_shapes=[pltpu.VMEM((np_, rows, quarter), f32)] * steps,
        ),
        compiler_params=pltpu.CompilerParams(vmem_limit_bytes=ADAM_MIB * MIB),
        cost_estimate=pl.CostEstimate(
            flops=np_ * nr * steps * 2 * rows * tokens * quarter, bytes_accessed=np_ * nr * rows * quarter * 8, transcendentals=0
        ),
    )(pos, coef, first_moment, second_moment, w, *args)


def coefficients(skipped):
    found = []
    for s in range(2):
        for scale in (1.0 / math.sqrt(D), 1.0 / math.sqrt(FF)):
            go = (beta_first, (1.0 - beta_first) * scale, beta_second, (1.0 - beta_second) * scale * scale, 1.0 - inner_rate * decay_rate, inner_rate)
            stay = (1.0, 0.0, 1.0, 0.0, 1.0, 0.0)
            found.append(jnp.where(skipped[s], jnp.array(stay, f32), jnp.array(go, f32)))
    return jnp.concatenate(found)


def round_of(weights, momentum, first_moment, second_moment, inputs, targets, overflow_step):
    _, rows, quarter = weights.shape
    zh, co = lax.axis_index("zh"), lax.axis_index("co")
    mine = 2 * zh + co

    def own_order(array):
        parts = [lax.dynamic_slice_in_dim(array, (mine ^ r) * quarter, quarter, axis=2) for r in range(4)]
        return jnp.concatenate(parts, axis=2)

    def partner(array):
        return lax.ppermute(array, "co", [(0, 1), (1, 0)])

    def across(array):
        return lax.ppermute(array, "zh", [(0, 1), (1, 0)])

    steps, tok, width = inputs.shape
    half = width // 2
    pair = collect(inputs, "zl")
    told = jnp.max(jnp.stack([(e == jnp.arange(128, dtype=jnp.int32)).astype(bf16) for e in around(overflow_step, "zl")]), axis=0)
    own = [weights[0:2].astype(bf16), weights[2:3].astype(bf16)]
    far = []
    for chunk in own:
        far.append(across(chunk))
    near = [partner(chunk) for chunk in own]
    both = [partner(chunk) for chunk in far]
    w = own + near + far + both

    inputs, targets, pair = own_order(inputs), own_order(targets), own_order(pair.reshape(2 * steps, tok, width))
    pair = pair.reshape(2, steps, tok, width)
    marks = jnp.broadcast_to(told.reshape(1, 1, 128), (2, tok, 128))
    low = jnp.concatenate([pair[:, k, :, :half] for k in range(steps)], axis=2)
    high = jnp.concatenate([pair[:, k, :, half:] for k in range(steps)] + [marks], axis=2)
    flat = [m.reshape(-1, m.shape[-1]) for m in (collect(low, "y"), collect(high, "x"))]
    pieces = around(flat[0], "x") + around(flat[1], "y")
    begin = steps * half
    marked = functools.reduce(jnp.maximum, [jnp.max(p[:, begin : begin + steps], axis=0) for p in pieces[4:]])
    coef = coefficients([marked[s] > 0 for s in range(steps)])
    pos = mine.reshape(1).astype(jnp.int32)
    first_moment = pltpu.with_memory_space_constraint(first_moment, pltpu.HBM)
    second_moment = pltpu.with_memory_space_constraint(second_moment, pltpu.HBM)
    at = jnp.stack([lax.axis_index("x"), lax.axis_index("y")]).astype(jnp.int32)

    xs, ys = [inputs[k] for k in range(steps)], [targets[k] for k in range(steps)]
    parts = []
    w_start = None
    for k in range(steps):
        x, gate, up, hidden, sums, *w0 = forward(at, k, pieces, w, rows)
        if k == 0:
            w = w_start = w0[0]
            sums, coef, xs, ys = lax.optimization_barrier((sums, coef, xs, ys))
        arrived = lax.all_to_all(sums.reshape(-1, tok, width), FSDP, 0, 0, tiled=True)
        copies = own_slopes(arrived, xs[k], ys[k])
        z = lax.all_to_all(copies, FSDP, 0, 0, tiled=True).reshape(-1, width)
        parts.append((x, z, slope_parts(z, w, gate, up, hidden)))
        if k == 0:
            w = adam(pos, coef, first_moment, second_moment, w, parts, (range(3), range(4)))
    arrived = []
    for p in (2, 0, 1):
        pair = adam(pos, coef, first_moment, second_moment, w_start, parts, ((p,), (3, 2)))
        joint = (pair[0, 1].astype(f32) + partner(pair[0, 0]).astype(f32)).astype(bf16)
        joint, pos = lax.optimization_barrier((joint, pos))
        arrived.append((p, across(joint)))
    rest = adam(pos, coef, first_moment, second_moment, w_start, parts, (range(3), (1, 0)))
    near_part = partner(rest[:, 0])
    arrived = jnp.stack([a for _, a in sorted(arrived, key=lambda e: e[0])])
    delta = (rest[:, 1].astype(f32) + near_part.astype(f32) + arrived.astype(f32)) / 4
    new_momentum = nesterov_coef * momentum + delta
    new_weights = weights - outer_rate * (delta + nesterov_coef * new_momentum)
    return (new_weights, new_momentum)


def solution(mesh):
    grid = Mesh(mesh.devices.reshape(2, 2, 4, 2, 4), ("zh", "co", "x", "zl", "y"))
    isl, fsdp = ("zh", "co"), ("x", "zl", "y")
    in_specs = (
        P(None, fsdp, isl),
        P(None, fsdp, isl),
        P(isl, None, fsdp, None),
        P(isl, None, fsdp, None),
        P(None, isl + fsdp, None),
        P(None, isl + fsdp, None),
        P(isl, fsdp),
    )
    out_specs = (P(None, fsdp, isl), P(None, fsdp, isl))
    return jax.shard_map(round_of, mesh=grid, in_specs=in_specs, out_specs=out_specs, check_vma=False)
```

```python
import functools
import math

import jax
import jax.numpy as jnp
from jax import lax
from jax.experimental import pallas as pl
from jax.experimental.pallas import tpu as pltpu
from jax.sharding import Mesh
from jax.sharding import PartitionSpec as P


D = 4096
FF = 7168

inner_rate = 0.02
beta_first = 0.9
beta_second = 0.95
epsilon = 1e-08
decay_rate = 0.1
outer_rate = 0.7
nesterov_coef = 0.9


bf16, f32 = jnp.bfloat16, jnp.float32

FSDP = ("x", "y", "zl")
SIZES = {"x": 4, "y": 4, "zl": 2}


def around(own, dim):
    n = SIZES[dim]
    return [own] + [lax.ppermute(own, dim, [(i, (i - s) % n) for i in range(n)]) for s in range(1, n)]


def collect(own, dim):
    n = SIZES[dim]
    blocks = around(own, dim)
    ring = jnp.stack(blocks + blocks[:-1])
    return lax.dynamic_slice_in_dim(ring, (n - lax.axis_index(dim)) % n, n, axis=0)


def contract_last(left, right):
    return lax.dot_general(left, right, (((1,), (1,)), ((), ())), preferred_element_type=f32)


VM = pl.BlockSpec(memory_space=pltpu.VMEM)
SM = pl.BlockSpec(memory_space=pltpu.SMEM)
MIB = 1 << 20
FORWARD_MIB, ADAM_MIB, SMALL_MIB = 6, 13, 4


def forward_kernel(n_w, at_ref, *refs):
    pieces, refs = refs[:8], refs[8:]
    w_refs, refs = refs[:n_w], refs[n_w:]
    x_out, gate_out, up_out, hidden_out, p_out = refs[:5]
    turn = refs[-1]
    quarter = x_out.shape[1] // 4

    def w(p, r):
        if n_w == 1:
            return w_refs[0][p, r]
        return w_refs[2 * r][p] if p < 2 else w_refs[2 * r + 1][0]

    plane = pieces[0].shape[0]
    block = plane // 4
    for a in range(4):
        source = slice(a % 2 * quarter, (a % 2 + 1) * quarter)
        cols = pl.ds(pl.multiple_of((at_ref[2] ^ a) * quarter, quarter), quarter)
        for s in range(4):
            if a < 2:
                row = pl.multiple_of(((at_ref[0] + s) % 4) * plane, plane)
                x_out[pl.ds(row, plane), cols] = pieces[s][:, source]
                continue
            for x in range(4):
                row = pl.multiple_of(x * plane + ((at_ref[1] + s) % 4) * block, block)
                x_out[pl.ds(row, block), cols] = pieces[4 + s][x * block : (x + 1) * block, source]
    if n_w > 1:
        for p in range(3):
            for r in range(4):
                refs[5][p, r] = w(p, r)
    gate, up = None, None
    for r in range(4):
        x = x_out[:, r * quarter : (r + 1) * quarter]
        g, u = contract_last(w(0, r), x), contract_last(w(1, r), x)
        gate = g if gate is None else gate + g
        up = u if up is None else up + u
    gate = gate * (1.0 / math.sqrt(D))
    up = up * (1.0 / math.sqrt(D))
    gate_out[...] = gate
    up_out[...] = up
    hidden = (gate * jax.nn.sigmoid(gate)) * up
    hidden_out[...] = hidden.astype(bf16)
    rows = hidden.shape[0]
    turn[...] = jnp.zeros_like(turn)
    turn[0:rows, :] = hidden
    turned = turn[...].T[:, 0:rows].astype(bf16)
    for r in range(4):
        part = jnp.dot(turned, w(2, r), preferred_element_type=f32)
        p_out[:, r * quarter : (r + 1) * quarter] = part.astype(bf16)


def forward(at, pieces, w, rows):
    first = isinstance(w, list)
    tokens, width = 4 * pieces[0].shape[0], 2 * pieces[0].shape[1]
    square = -(-max(rows, tokens) // 128) * 128
    small = pltpu.VMEM((rows, tokens), f32)
    wide = jax.ShapeDtypeStruct((tokens, width), bf16)
    outs = [pltpu.VMEM((tokens, width), bf16), small, small, pltpu.VMEM((rows, tokens), bf16), wide]
    if first:
        outs.append(pltpu.VMEM((3, 4, rows, width // 4), bf16))
    weights = w if first else [w]
    return pl.pallas_call(
        functools.partial(forward_kernel, len(weights)),
        out_shape=outs,
        in_specs=[SM] + [VM] * (8 + len(weights)),
        out_specs=[VM] * len(outs),
        scratch_shapes=[pltpu.VMEM((square, tokens), f32)],
        compiler_params=pltpu.CompilerParams(vmem_limit_bytes=FORWARD_MIB * MIB),
        cost_estimate=pl.CostEstimate(flops=6 * rows * tokens * width, bytes_accessed=8 << 20, transcendentals=0),
        name="forward0" if first else "forward1",
    )(at, *pieces, *weights)


def slopes_kernel(scale, parts_ref, x_ref, y_ref, out_ref):
    width = x_ref.shape[1]
    lanes = min(512, width)
    for low in range(0, width, lanes):
        cols = slice(low, low + lanes)
        total = parts_ref[0, :, cols].astype(f32)
        for k in range(1, parts_ref.shape[0]):
            total = total + parts_ref[k, :, cols].astype(f32)
        outputs = x_ref[:, cols].astype(f32) + total * (1.0 / math.sqrt(FF))
        slopes = ((outputs - y_ref[:, cols].astype(f32)) * scale).astype(bf16)
        for k in range(out_ref.shape[0]):
            out_ref[k, :, cols] = slopes


def own_slopes(parts, x, y):
    n, tok, width = parts.shape
    return pl.pallas_call(
        functools.partial(slopes_kernel, 1.0 / (n * tok)),
        out_shape=jax.ShapeDtypeStruct(parts.shape, bf16),
        in_specs=[VM, VM, VM],
        out_specs=VM,
        compiler_params=pltpu.CompilerParams(vmem_limit_bytes=SMALL_MIB * MIB),
        cost_estimate=pl.CostEstimate(flops=n * tok * width, bytes_accessed=4 * n * tok * width, transcendentals=0),
        name="own_slopes",
    )(parts, x, y)


def slope_kernel(z_ref, w_ref, gate_ref, up_ref, hidden_ref, s_out):
    quarter = w_ref.shape[-1]
    slope = None
    for r in range(4):
        part = contract_last(w_ref[2, r], z_ref[:, r * quarter : (r + 1) * quarter])
        slope = part if slope is None else slope + part
    slope = slope * (1.0 / math.sqrt(FF))
    gate = gate_ref[...]
    sig = jax.nn.sigmoid(gate)
    s_out[0] = (slope * up_ref[...] * (sig * (1.0 + gate * (1.0 - sig)))).astype(bf16)
    s_out[1] = (slope * (gate * sig)).astype(bf16)
    s_out[2] = hidden_ref[...]


def slope_parts(z, w, gate, up, hidden):
    rows, tokens = gate.shape
    width = z.shape[1]
    return pl.pallas_call(
        slope_kernel,
        out_shape=pltpu.VMEM((3, rows, tokens), bf16),
        in_specs=[VM] * 5,
        out_specs=VM,
        compiler_params=pltpu.CompilerParams(vmem_limit_bytes=SMALL_MIB * MIB),
        cost_estimate=pl.CostEstimate(flops=2 * rows * tokens * width, bytes_accessed=4 << 20, transcendentals=0),
        name="slope_parts",
    )(z, w, gate, up, hidden)


def adam_step(m, v, c, g, k):
    m = k[0] * m + k[1] * g
    v = k[2] * v + k[3] * (g * g)
    root = v * lax.rsqrt(v)
    c = k[4] * c - k[5] * (m / (root + epsilon))
    return m, v, c


def adam_kernel(steps, ps, r_of, lanes, pos, coef, m_ref, v_ref, w_ref, *refs):
    ins = [refs[3 * s : 3 * s + 3] for s in range(steps)]
    out_ref = refs[3 * steps]
    g_refs = refs[3 * steps + 1 :]
    i = pl.program_id(0)
    r = r_of(i)
    _, rows, quarter = g_refs[0].shape
    across = pl.ds(pl.multiple_of(r * quarter, quarter), quarter)
    for n, p in enumerate(ps):
        for s in range(steps):
            x_ref, z_ref, s_ref = ins[s]
            right = (x_ref if p < 2 else z_ref)[:, across]
            g_refs[s][n] = jnp.dot(s_ref[p], right, preferred_element_type=f32)
    step_rows = 16
    for n, p in enumerate(ps):
        ks = [[coef[12 * s + (6 if p == 2 else 0) + j] for j in range(6)] for s in range(steps)]

        @pl.loop(0, rows // step_rows, unroll=2 if (rows // step_rows) % 2 == 0 else 1)
        def _(k, n=n, p=p, ks=ks):
            at = pl.ds(pl.multiple_of(k * step_rows, step_rows), step_rows)
            for low in range(0, quarter, lanes):
                cols = slice(low, low + lanes)
                m = m_ref[0, n, at, cols].astype(f32)
                v = v_ref[0, n, at, cols].astype(f32)
                start = w_ref[p, r, at, cols].astype(f32)
                c = start
                for s in range(steps):
                    m, v, c = adam_step(m, v, c, g_refs[s][n, at, cols], ks[s])
                out_ref[n, i, at, cols] = (c if steps == 1 else start - c).astype(bf16)


def adam(pos, coef, first_moment, second_moment, w, parts, tiles):
    ps, rs = list(tiles[0]), list(tiles[1])
    steps = len(parts)
    rows, quarter = w.shape[2:]
    tokens = parts[0][0].shape[0]
    np_, nr = len(ps), len(rs)
    stride = rs[1] - rs[0] if nr > 1 else 0
    assert rs == [rs[0] + stride * k for k in range(nr)] and ps == list(range(ps[0], ps[0] + np_)) and ps[0] % np_ == 0

    def r_of(i):
        return rs[0] + stride * i

    moment = pl.BlockSpec((1, np_, rows, quarter), lambda i, pos: (0, ps[0] // np_, 0, r_of(i) ^ pos[0]))
    args = [a for part in parts for a in part]
    return pl.pallas_call(
        functools.partial(adam_kernel, steps, ps, r_of, min(512, quarter)),
        out_shape=pltpu.VMEM((np_, nr, rows, quarter), bf16),
        grid_spec=pltpu.PrefetchScalarGridSpec(
            num_scalar_prefetch=1,
            grid=(nr,),
            in_specs=[SM, moment, moment, VM] + [VM] * (3 * steps),
            out_specs=VM,
            scratch_shapes=[pltpu.VMEM((np_, rows, quarter), f32)] * steps,
        ),
        compiler_params=pltpu.CompilerParams(vmem_limit_bytes=ADAM_MIB * MIB),
        cost_estimate=pl.CostEstimate(
            flops=np_ * nr * steps * 2 * rows * tokens * quarter, bytes_accessed=np_ * nr * rows * quarter * 8, transcendentals=0
        ),
    )(pos, coef, first_moment, second_moment, w, *args)


def settle_kernel(w_ref, m_ref, own_ref, near_ref, far_ref, *refs):
    w_out, m_out = refs[-2:]
    total = own_ref[0, 0].astype(f32) + near_ref[0].astype(f32) + far_ref[...].astype(f32)
    delta = total * 0.25
    new_momentum = nesterov_coef * m_ref[0] + delta
    m_out[0] = new_momentum
    w_out[0] = w_ref[0] - outer_rate * (delta + nesterov_coef * new_momentum)


def settle(p, weights, momentum, own, near, far, before):
    _, rows, quarter = weights.shape
    half = rows // 2
    block = pl.BlockSpec((1, half, quarter), lambda i: (p, i, 0))
    shape = jax.ShapeDtypeStruct(weights.shape, f32)
    return pl.pallas_call(
        settle_kernel,
        grid=(2,),
        out_shape=[shape, shape],
        in_specs=[
            block,
            block,
            pl.BlockSpec((1, 1, half, quarter), lambda i: (p, 1, i, 0)),
            block,
            pl.BlockSpec((half, quarter), lambda i: (i, 0)),
        ]
        + [pl.BlockSpec(memory_space=pl.ANY)] * len(before),
        out_specs=[block, block],
        input_output_aliases={5 + k: k for k in range(len(before))},
        compiler_params=pltpu.CompilerParams(vmem_limit_bytes=12 * MIB),
    )(weights, momentum, own, near, far, *before)


def coefficients(skipped):
    found = []
    for s in range(2):
        for scale in (1.0 / math.sqrt(D), 1.0 / math.sqrt(FF)):
            go = (beta_first, (1.0 - beta_first) * scale, beta_second, (1.0 - beta_second) * scale * scale, 1.0 - inner_rate * decay_rate, inner_rate)
            stay = (1.0, 0.0, 1.0, 0.0, 1.0, 0.0)
            found.append(jnp.where(skipped[s], jnp.array(stay, f32), jnp.array(go, f32)))
    return jnp.concatenate(found)


def round_of(weights, momentum, first_moment, second_moment, inputs, targets, overflow_step):
    _, rows, quarter = weights.shape
    zh, co = lax.axis_index("zh"), lax.axis_index("co")
    mine = 2 * zh + co

    def own_order(array):
        parts = [lax.dynamic_slice_in_dim(array, (mine ^ r) * quarter, quarter, axis=2) for r in range(4)]
        return jnp.concatenate(parts, axis=2)

    def partner(array):
        return lax.ppermute(array, "co", [(0, 1), (1, 0)])

    def across(array):
        return lax.ppermute(array, "zh", [(0, 1), (1, 0)])

    steps, tok, width = inputs.shape
    half = width // 2
    pair = collect(inputs, "zl")
    told = jnp.max(jnp.stack([(e == jnp.arange(128, dtype=jnp.int32)).astype(bf16) for e in around(overflow_step, "zl")]), axis=0)
    own = [weights[0:2].astype(bf16), weights[2:3].astype(bf16)]
    far = []
    for chunk in own:
        far.append(across(chunk))
    near = [partner(chunk) for chunk in own]
    both = [partner(chunk) for chunk in far]
    w = own + near + far + both

    marks = jnp.broadcast_to(told.reshape(1, 1, 128), (2, tok, 128))
    low = jnp.concatenate([pair[:, k, :, :half] for k in range(steps)], axis=2)
    high = jnp.concatenate([pair[:, 0, :, half:], marks] + [pair[:, k, :, half:] for k in range(1, steps)], axis=2)
    flat = [m.reshape(-1, m.shape[-1]) for m in (collect(low, "y"), collect(high, "x"))]
    pieces = []
    for k in range(steps):
        start, stop = (k * half + (128 if k else 0), (k + 1) * half + 128)
        pieces.append(around(flat[0][:, k * half : (k + 1) * half], "x") + around(flat[1][:, start:stop], "y"))
    inputs, targets = own_order(inputs), own_order(targets)
    marked = functools.reduce(jnp.maximum, [jnp.max(p[:, half : half + steps], axis=0) for p in pieces[0][4:]])
    coef = coefficients([marked[s] > 0 for s in range(steps)])
    pos = mine.reshape(1).astype(jnp.int32)
    first_moment = pltpu.with_memory_space_constraint(first_moment, pltpu.HBM)
    second_moment = pltpu.with_memory_space_constraint(second_moment, pltpu.HBM)
    at = jnp.stack([lax.axis_index("x"), lax.axis_index("y"), mine]).astype(jnp.int32)

    xs, ys = [inputs[k] for k in range(steps)], [targets[k] for k in range(steps)]
    parts = []
    w_start = None
    for k in range(steps):
        x, gate, up, hidden, sums, *w0 = forward(at, pieces[k], w, rows)
        if k == 0:
            w = w_start = w0[0]
            sums, coef, xs, ys = lax.optimization_barrier((sums, coef, xs, ys))
        arrived = lax.all_to_all(sums.reshape(-1, tok, width), FSDP, 0, 0, tiled=True)
        copies = own_slopes(arrived, xs[k], ys[k])
        z = lax.all_to_all(copies, FSDP, 0, 0, tiled=True).reshape(-1, width)
        parts.append((x, z, slope_parts(z, w, gate, up, hidden)))
        if k == 0:
            w = adam(pos, coef, first_moment, second_moment, w, parts, (range(3), range(4)))
    arrived = []
    for p in (2, 0, 1):
        pair = adam(pos, coef, first_moment, second_moment, w_start, parts, ((p,), (3, 2)))
        joint = (pair[0, 1].astype(f32) + partner(pair[0, 0]).astype(f32)).astype(bf16)
        joint, pos = lax.optimization_barrier((joint, pos))
        arrived.append((p, across(joint)))
    rest = adam(pos, coef, first_moment, second_moment, w_start, parts, (range(3), (1, 0)))
    near_part = partner(rest[:, 0])
    result = ()
    for p, far_part in arrived:
        result = settle(p, weights, momentum, rest, near_part, far_part, result)
    return tuple(result)


def solution(mesh):
    grid = Mesh(mesh.devices.reshape(2, 2, 4, 2, 4), ("zh", "co", "x", "zl", "y"))
    isl, fsdp = ("zh", "co"), ("x", "zl", "y")
    in_specs = (
        P(None, fsdp, isl),
        P(None, fsdp, isl),
        P(isl, None, fsdp, None),
        P(isl, None, fsdp, None),
        P(None, isl + fsdp, None),
        P(None, isl + fsdp, None),
        P(isl, fsdp),
    )
    out_specs = (P(None, fsdp, isl), P(None, fsdp, isl))
    return jax.shard_map(round_of, mesh=grid, in_specs=in_specs, out_specs=out_specs, check_vma=False)
```

```python
import functools
import math

import jax
import jax.numpy as jnp
from jax import lax
from jax.experimental import pallas as pl
from jax.experimental.pallas import tpu as pltpu
from jax.sharding import Mesh
from jax.sharding import PartitionSpec as P


D = 4096
FF = 7168

inner_rate = 0.02
beta_first = 0.9
beta_second = 0.95
epsilon = 1e-08
decay_rate = 0.1
outer_rate = 0.7
nesterov_coef = 0.9


bf16, f32 = jnp.bfloat16, jnp.float32

FSDP = ("x", "y", "zl")
SIZES = {"x": 4, "y": 4, "zl": 2}


def around(own, dim):
    n = SIZES[dim]
    return [own] + [lax.ppermute(own, dim, [(i, (i - s) % n) for i in range(n)]) for s in range(1, n)]


def collect(own, dim):
    n = SIZES[dim]
    blocks = around(own, dim)
    ring = jnp.stack(blocks + blocks[:-1])
    return lax.dynamic_slice_in_dim(ring, (n - lax.axis_index(dim)) % n, n, axis=0)


def contract_last(left, right):
    return lax.dot_general(left, right, (((1,), (1,)), ((), ())), preferred_element_type=f32)


VM = pl.BlockSpec(memory_space=pltpu.VMEM)
SM = pl.BlockSpec(memory_space=pltpu.SMEM)
MIB = 1 << 20
FORWARD_MIB, ADAM_MIB, SMALL_MIB = 6, 13, 4


def forward_kernel(n_w, at_ref, *refs):
    pieces, refs = refs[:8], refs[8:]
    w_refs, refs = refs[:n_w], refs[n_w:]
    x_out, gate_out, up_out, hidden_out, p_out = refs[:5]
    turn = refs[-1]
    quarter = x_out.shape[1] // 4

    def w(p, r):
        if n_w == 1:
            return w_refs[0][p, r]
        return w_refs[2 * r][p] if p < 2 else w_refs[2 * r + 1][0]

    plane = pieces[0].shape[0]
    block = plane // 4
    for a in range(4):
        source = slice(a % 2 * quarter, (a % 2 + 1) * quarter)
        cols = pl.ds(pl.multiple_of((at_ref[2] ^ a) * quarter, quarter), quarter)
        for s in range(4):
            if a < 2:
                row = pl.multiple_of(((at_ref[0] + s) % 4) * plane, plane)
                x_out[pl.ds(row, plane), cols] = pieces[s][:, source]
                continue
            for x in range(4):
                row = pl.multiple_of(x * plane + ((at_ref[1] + s) % 4) * block, block)
                x_out[pl.ds(row, block), cols] = pieces[4 + s][x * block : (x + 1) * block, source]
    if n_w > 1:
        for p in range(3):
            for r in range(4):
                refs[5][p, r] = w(p, r)
    gate, up = None, None
    for r in range(4):
        x = x_out[:, r * quarter : (r + 1) * quarter]
        g, u = contract_last(w(0, r), x), contract_last(w(1, r), x)
        gate = g if gate is None else gate + g
        up = u if up is None else up + u
    gate = gate * (1.0 / math.sqrt(D))
    up = up * (1.0 / math.sqrt(D))
    gate_out[...] = gate
    up_out[...] = up
    hidden = (gate * jax.nn.sigmoid(gate)) * up
    hidden_out[...] = hidden.astype(bf16)
    rows = hidden.shape[0]
    turn[...] = jnp.zeros_like(turn)
    turn[0:rows, :] = hidden
    turned = turn[...].T[:, 0:rows].astype(bf16)
    for r in range(4):
        part = jnp.dot(turned, w(2, r), preferred_element_type=f32)
        p_out[:, r * quarter : (r + 1) * quarter] = part.astype(bf16)


def forward(at, pieces, w, rows):
    first = isinstance(w, list)
    tokens, width = 4 * pieces[0].shape[0], 2 * pieces[0].shape[1]
    square = -(-max(rows, tokens) // 128) * 128
    small = pltpu.VMEM((rows, tokens), f32)
    wide = jax.ShapeDtypeStruct((tokens, width), bf16)
    outs = [pltpu.VMEM((tokens, width), bf16), small, small, pltpu.VMEM((rows, tokens), bf16), wide]
    if first:
        outs.append(pltpu.VMEM((3, 4, rows, width // 4), bf16))
    weights = w if first else [w]
    return pl.pallas_call(
        functools.partial(forward_kernel, len(weights)),
        out_shape=outs,
        in_specs=[SM] + [VM] * (8 + len(weights)),
        out_specs=[VM] * len(outs),
        scratch_shapes=[pltpu.VMEM((square, tokens), f32)],
        compiler_params=pltpu.CompilerParams(vmem_limit_bytes=FORWARD_MIB * MIB),
        cost_estimate=pl.CostEstimate(flops=6 * rows * tokens * width, bytes_accessed=8 << 20, transcendentals=0),
        name="forward0" if first else "forward1",
    )(at, *pieces, *weights)


def slopes_kernel(scale, parts_ref, x_ref, y_ref, out_ref):
    width = x_ref.shape[1]
    lanes = min(512, width)
    for low in range(0, width, lanes):
        cols = slice(low, low + lanes)
        total = parts_ref[0, :, cols].astype(f32)
        for k in range(1, parts_ref.shape[0]):
            total = total + parts_ref[k, :, cols].astype(f32)
        outputs = x_ref[:, cols].astype(f32) + total * (1.0 / math.sqrt(FF))
        slopes = ((outputs - y_ref[:, cols].astype(f32)) * scale).astype(bf16)
        for k in range(out_ref.shape[0]):
            out_ref[k, :, cols] = slopes


def own_slopes(parts, x, y):
    n, tok, width = parts.shape
    return pl.pallas_call(
        functools.partial(slopes_kernel, 1.0 / (n * tok)),
        out_shape=jax.ShapeDtypeStruct(parts.shape, bf16),
        in_specs=[VM, VM, VM],
        out_specs=VM,
        compiler_params=pltpu.CompilerParams(vmem_limit_bytes=SMALL_MIB * MIB),
        cost_estimate=pl.CostEstimate(flops=n * tok * width, bytes_accessed=4 * n * tok * width, transcendentals=0),
        name="own_slopes",
    )(parts, x, y)


def slope_kernel(z_ref, w_ref, gate_ref, up_ref, hidden_ref, s_out):
    quarter = w_ref.shape[-1]
    slope = None
    for r in range(4):
        part = contract_last(w_ref[2, r], z_ref[:, r * quarter : (r + 1) * quarter])
        slope = part if slope is None else slope + part
    slope = slope * (1.0 / math.sqrt(FF))
    gate = gate_ref[...]
    sig = jax.nn.sigmoid(gate)
    s_out[0] = (slope * up_ref[...] * (sig * (1.0 + gate * (1.0 - sig)))).astype(bf16)
    s_out[1] = (slope * (gate * sig)).astype(bf16)
    s_out[2] = hidden_ref[...]


def slope_parts(z, w, gate, up, hidden):
    rows, tokens = gate.shape
    width = z.shape[1]
    return pl.pallas_call(
        slope_kernel,
        out_shape=pltpu.VMEM((3, rows, tokens), bf16),
        in_specs=[VM] * 5,
        out_specs=VM,
        compiler_params=pltpu.CompilerParams(vmem_limit_bytes=SMALL_MIB * MIB),
        cost_estimate=pl.CostEstimate(flops=2 * rows * tokens * width, bytes_accessed=4 << 20, transcendentals=0),
        name="slope_parts",
    )(z, w, gate, up, hidden)


def adam_step(m, v, c, g, k):
    m = k[0] * m + k[1] * g
    v = k[2] * v + k[3] * (g * g)
    root = v * lax.rsqrt(v)
    c = k[4] * c - k[5] * (m / (root + epsilon))
    return m, v, c


def adam_kernel(steps, ps, r_of, lanes, pos, coef, m_ref, v_ref, w_ref, *refs):
    ins = [refs[3 * s : 3 * s + 3] for s in range(steps)]
    out_ref = refs[3 * steps]
    g_refs = refs[3 * steps + 1 :]
    i = pl.program_id(0)
    r = r_of(i)
    _, rows, quarter = g_refs[0].shape
    across = pl.ds(pl.multiple_of(r * quarter, quarter), quarter)
    for n, p in enumerate(ps):
        for s in range(steps):
            x_ref, z_ref, s_ref = ins[s]
            right = (x_ref if p < 2 else z_ref)[:, across]
            g_refs[s][n] = jnp.dot(s_ref[p], right, preferred_element_type=f32)
    step_rows = 16
    for n, p in enumerate(ps):
        ks = [[coef[12 * s + (6 if p == 2 else 0) + j] for j in range(6)] for s in range(steps)]

        @pl.loop(0, rows // step_rows, unroll=2 if (rows // step_rows) % 2 == 0 else 1)
        def _(k, n=n, p=p, ks=ks):
            at = pl.ds(pl.multiple_of(k * step_rows, step_rows), step_rows)
            for low in range(0, quarter, lanes):
                cols = slice(low, low + lanes)
                m = m_ref[0, n, at, cols].astype(f32)
                v = v_ref[0, n, at, cols].astype(f32)
                start = w_ref[p, r, at, cols].astype(f32)
                c = start
                for s in range(steps):
                    m, v, c = adam_step(m, v, c, g_refs[s][n, at, cols], ks[s])
                out_ref[n, i, at, cols] = (c if steps == 1 else start - c).astype(bf16)


def adam(pos, coef, first_moment, second_moment, w, parts, tiles):
    ps, rs = list(tiles[0]), list(tiles[1])
    steps = len(parts)
    rows, quarter = w.shape[2:]
    tokens = parts[0][0].shape[0]
    np_, nr = len(ps), len(rs)
    stride = rs[1] - rs[0] if nr > 1 else 0
    assert rs == [rs[0] + stride * k for k in range(nr)] and ps == list(range(ps[0], ps[0] + np_)) and ps[0] % np_ == 0

    def r_of(i):
        return rs[0] + stride * i

    moment = pl.BlockSpec((1, np_, rows, quarter), lambda i, pos: (0, ps[0] // np_, 0, r_of(i) ^ pos[0]))
    args = [a for part in parts for a in part]
    return pl.pallas_call(
        functools.partial(adam_kernel, steps, ps, r_of, min(512, quarter)),
        out_shape=pltpu.VMEM((np_, nr, rows, quarter), bf16),
        grid_spec=pltpu.PrefetchScalarGridSpec(
            num_scalar_prefetch=1,
            grid=(nr,),
            in_specs=[SM, moment, moment, VM] + [VM] * (3 * steps),
            out_specs=VM,
            scratch_shapes=[pltpu.VMEM((np_, rows, quarter), f32)] * steps,
        ),
        compiler_params=pltpu.CompilerParams(vmem_limit_bytes=ADAM_MIB * MIB),
        cost_estimate=pl.CostEstimate(
            flops=np_ * nr * steps * 2 * rows * tokens * quarter, bytes_accessed=np_ * nr * rows * quarter * 8, transcendentals=0
        ),
    )(pos, coef, first_moment, second_moment, w, *args)


def settle_kernel(w_ref, m_ref, own_ref, near_ref, far_ref, *refs):
    w_out, m_out = refs[-2:]
    total = own_ref[0, 0].astype(f32) + near_ref[0].astype(f32) + far_ref[...].astype(f32)
    delta = total * 0.25
    new_momentum = nesterov_coef * m_ref[0] + delta
    m_out[0] = new_momentum
    w_out[0] = w_ref[0] - outer_rate * (delta + nesterov_coef * new_momentum)


def settle(p, weights, momentum, own, near, far, before):
    _, rows, quarter = weights.shape
    half = rows // 2
    block = pl.BlockSpec((1, half, quarter), lambda i: (p, i, 0))
    shape = jax.ShapeDtypeStruct(weights.shape, f32)
    return pl.pallas_call(
        settle_kernel,
        grid=(2,),
        out_shape=[shape, shape],
        in_specs=[
            block,
            block,
            pl.BlockSpec((1, 1, half, quarter), lambda i: (p, 0, i, 0)),
            block,
            pl.BlockSpec((half, quarter), lambda i: (i, 0)),
        ]
        + [pl.BlockSpec(memory_space=pl.ANY)] * len(before),
        out_specs=[block, block],
        input_output_aliases={5 + k: k for k in range(len(before))},
        compiler_params=pltpu.CompilerParams(vmem_limit_bytes=12 * MIB),
    )(weights, momentum, own, near, far, *before)


def coefficients(skipped):
    found = []
    for s in range(2):
        for scale in (1.0 / math.sqrt(D), 1.0 / math.sqrt(FF)):
            go = (beta_first, (1.0 - beta_first) * scale, beta_second, (1.0 - beta_second) * scale * scale, 1.0 - inner_rate * decay_rate, inner_rate)
            stay = (1.0, 0.0, 1.0, 0.0, 1.0, 0.0)
            found.append(jnp.where(skipped[s], jnp.array(stay, f32), jnp.array(go, f32)))
    return jnp.concatenate(found)


def round_of(weights, momentum, first_moment, second_moment, inputs, targets, overflow_step):
    _, rows, quarter = weights.shape
    zh, co = lax.axis_index("zh"), lax.axis_index("co")
    mine = 2 * zh + co

    def own_order(array):
        parts = [lax.dynamic_slice_in_dim(array, (mine ^ r) * quarter, quarter, axis=2) for r in range(4)]
        return jnp.concatenate(parts, axis=2)

    def partner(array):
        return lax.ppermute(array, "co", [(0, 1), (1, 0)])

    def across(array):
        return lax.ppermute(array, "zh", [(0, 1), (1, 0)])

    steps, tok, width = inputs.shape
    half = width // 2
    pair = collect(inputs, "zl")
    told = jnp.max(jnp.stack([(e == jnp.arange(128, dtype=jnp.int32)).astype(bf16) for e in around(overflow_step, "zl")]), axis=0)
    own = [weights[0:2].astype(bf16), weights[2:3].astype(bf16)]
    far = []
    for chunk in own:
        far.append(across(chunk))
    near = []
    for chunk in own:
        near.append(partner(chunk))

    marks = jnp.broadcast_to(told.reshape(1, 1, 128), (2, tok, 128))
    low = jnp.concatenate([pair[:, k, :, :half] for k in range(steps)], axis=2)
    high = jnp.concatenate([pair[:, 0, :, half:], marks] + [pair[:, k, :, half:] for k in range(1, steps)], axis=2)
    flat = [m.reshape(-1, m.shape[-1]) for m in (collect(low, "y"), collect(high, "x"))]
    pieces = []
    for k in range(steps):
        start, stop = (k * half + (128 if k else 0), (k + 1) * half + 128)
        pieces.append(around(flat[0][:, k * half : (k + 1) * half], "x") + around(flat[1][:, start:stop], "y"))
    inputs, targets, far[1] = lax.optimization_barrier((inputs, targets, far[1]))
    inputs, targets = own_order(inputs), own_order(targets)
    marked = functools.reduce(jnp.maximum, [jnp.max(p[:, half : half + steps], axis=0) for p in pieces[0][4:]])
    coef = coefficients([marked[s] > 0 for s in range(steps)])
    pos = mine.reshape(1).astype(jnp.int32)
    first_moment = pltpu.with_memory_space_constraint(first_moment, pltpu.HBM)
    second_moment = pltpu.with_memory_space_constraint(second_moment, pltpu.HBM)
    at = jnp.stack([lax.axis_index("x"), lax.axis_index("y"), mine]).astype(jnp.int32)

    both = [partner(chunk) for chunk in far]
    w = own + near + far + both
    xs, ys = [inputs[k] for k in range(steps)], [targets[k] for k in range(steps)]
    parts = []
    w_start = None
    for k in range(steps):
        x, gate, up, hidden, sums, *w0 = forward(at, pieces[k], w, rows)
        if k == 0:
            w = w_start = w0[0]
            sums, coef, xs, ys = lax.optimization_barrier((sums, coef, xs, ys))
        arrived = lax.all_to_all(sums.reshape(-1, tok, width), FSDP, 0, 0, tiled=True)
        copies = own_slopes(arrived, xs[k], ys[k])
        z = lax.all_to_all(copies, FSDP, 0, 0, tiled=True).reshape(-1, width)
        parts.append((x, z, slope_parts(z, w, gate, up, hidden)))
        if k == 0:
            w = adam(pos, coef, first_moment, second_moment, w, parts, (range(3), range(4)))
    arrived = []
    state = (first_moment, second_moment, w_start, parts)
    for p in (2, 0, 1):
        if p == 2:
            out = adam(pos, coef, *state, ((p,), (3,)))[0, 0]
            handed = partner(out)
            kept = adam(pos, coef, *state, ((p,), (2,)))[0, 0]
        else:
            pair = adam(pos, coef, *state, ((p,), (3, 2)))
            handed, kept = partner(pair[0, 0]), pair[0, 1]
        joint = (kept.astype(f32) + handed.astype(f32)).astype(bf16)
        joint, pos = lax.optimization_barrier((joint, pos))
        arrived.append((p, across(joint)))
    beside = adam(pos, coef, *state, (range(3), (1,)))
    near_part = partner(beside[:, 0])
    rest = adam(pos, coef, *state, (range(3), (0,)))
    result = ()
    for p, far_part in arrived:
        result = settle(p, weights, momentum, rest, near_part, far_part, result)
    return tuple(result)


def solution(mesh):
    grid = Mesh(mesh.devices.reshape(2, 2, 4, 2, 4), ("zh", "co", "x", "zl", "y"))
    isl, fsdp = ("zh", "co"), ("x", "zl", "y")
    in_specs = (
        P(None, fsdp, isl),
        P(None, fsdp, isl),
        P(isl, None, fsdp, None),
        P(isl, None, fsdp, None),
        P(None, isl + fsdp, None),
        P(None, isl + fsdp, None),
        P(isl, fsdp),
    )
    out_specs = (P(None, fsdp, isl), P(None, fsdp, isl))
    return jax.shard_map(round_of, mesh=grid, in_specs=in_specs, out_specs=out_specs, check_vma=False)
```

```python
import functools
import math

import jax
import jax.numpy as jnp
from jax import lax
from jax.experimental import pallas as pl
from jax.experimental.pallas import tpu as pltpu
from jax.sharding import Mesh
from jax.sharding import PartitionSpec as P


D = 4096
FF = 7168

inner_rate = 0.02
beta_first = 0.9
beta_second = 0.95
epsilon = 1e-08
decay_rate = 0.1
outer_rate = 0.7
nesterov_coef = 0.9


bf16, f32 = jnp.bfloat16, jnp.float32

FSDP = ("x", "y", "zl")
SIZES = {"x": 4, "y": 4, "zl": 2}


def around(own, dim):
    n = SIZES[dim]
    return [own] + [lax.ppermute(own, dim, [(i, (i - s) % n) for i in range(n)]) for s in range(1, n)]


def collect(own, dim):
    n = SIZES[dim]
    blocks = around(own, dim)
    ring = jnp.stack(blocks + blocks[:-1])
    return lax.dynamic_slice_in_dim(ring, (n - lax.axis_index(dim)) % n, n, axis=0)


def contract_last(left, right):
    return lax.dot_general(left, right, (((1,), (1,)), ((), ())), preferred_element_type=f32)


VM = pl.BlockSpec(memory_space=pltpu.VMEM)
SM = pl.BlockSpec(memory_space=pltpu.SMEM)
MIB = 1 << 20
FORWARD_MIB, ADAM_MIB, SMALL_MIB = 6, 13, 4


def forward_kernel(n_w, at_ref, *refs):
    pieces, refs = refs[:8], refs[8:]
    w_refs, refs = refs[:n_w], refs[n_w:]
    x_out, gate_out, up_out, hidden_out, p_out = refs[:5]
    turn = refs[-1]
    quarter = x_out.shape[1] // 4

    def w(p, r):
        if n_w == 1:
            return w_refs[0][p, r]
        return w_refs[2 * r][p] if p < 2 else w_refs[2 * r + 1][0]

    plane = pieces[0].shape[0]
    block = plane // 4
    for a in range(4):
        source = slice(a % 2 * quarter, (a % 2 + 1) * quarter)
        cols = pl.ds(pl.multiple_of((at_ref[2] ^ a) * quarter, quarter), quarter)
        for s in range(4):
            if a < 2:
                row = pl.multiple_of(((at_ref[0] + s) % 4) * plane, plane)
                x_out[pl.ds(row, plane), cols] = pieces[s][:, source]
                continue
            for x in range(4):
                row = pl.multiple_of(x * plane + ((at_ref[1] + s) % 4) * block, block)
                x_out[pl.ds(row, block), cols] = pieces[4 + s][x * block : (x + 1) * block, source]
    if n_w > 1:
        for p in range(3):
            for r in range(4):
                refs[5][p, r] = w(p, r)
    gate, up = None, None
    for r in range(4):
        x = x_out[:, r * quarter : (r + 1) * quarter]
        g, u = contract_last(w(0, r), x), contract_last(w(1, r), x)
        gate = g if gate is None else gate + g
        up = u if up is None else up + u
    gate = gate * (1.0 / math.sqrt(D))
    up = up * (1.0 / math.sqrt(D))
    gate_out[...] = gate
    up_out[...] = up
    hidden = (gate * jax.nn.sigmoid(gate)) * up
    hidden_out[...] = hidden.astype(bf16)
    rows = hidden.shape[0]
    turn[...] = jnp.zeros_like(turn)
    turn[0:rows, :] = hidden
    turned = turn[...].T[:, 0:rows].astype(bf16)
    for r in range(4):
        part = jnp.dot(turned, w(2, r), preferred_element_type=f32)
        p_out[:, r * quarter : (r + 1) * quarter] = part.astype(bf16)


def forward(at, pieces, w, rows):
    first = isinstance(w, list)
    tokens, width = 4 * pieces[0].shape[0], 2 * pieces[0].shape[1]
    square = -(-max(rows, tokens) // 128) * 128
    small = pltpu.VMEM((rows, tokens), f32)
    wide = jax.ShapeDtypeStruct((tokens, width), bf16)
    outs = [pltpu.VMEM((tokens, width), bf16), small, small, pltpu.VMEM((rows, tokens), bf16), wide]
    if first:
        outs.append(pltpu.VMEM((3, 4, rows, width // 4), bf16))
    weights = w if first else [w]
    return pl.pallas_call(
        functools.partial(forward_kernel, len(weights)),
        out_shape=outs,
        in_specs=[SM] + [VM] * (8 + len(weights)),
        out_specs=[VM] * len(outs),
        scratch_shapes=[pltpu.VMEM((square, tokens), f32)],
        compiler_params=pltpu.CompilerParams(vmem_limit_bytes=FORWARD_MIB * MIB),
        cost_estimate=pl.CostEstimate(flops=6 * rows * tokens * width, bytes_accessed=8 << 20, transcendentals=0),
        name="forward0" if first else "forward1",
    )(at, *pieces, *weights)


def slopes_kernel(scale, parts_ref, x_ref, y_ref, out_ref):
    width = x_ref.shape[1]
    lanes = min(512, width)
    for low in range(0, width, lanes):
        cols = slice(low, low + lanes)
        total = parts_ref[0, :, cols].astype(f32)
        for k in range(1, parts_ref.shape[0]):
            total = total + parts_ref[k, :, cols].astype(f32)
        outputs = x_ref[:, cols].astype(f32) + total * (1.0 / math.sqrt(FF))
        slopes = ((outputs - y_ref[:, cols].astype(f32)) * scale).astype(bf16)
        for k in range(out_ref.shape[0]):
            out_ref[k, :, cols] = slopes


def own_slopes(parts, x, y):
    n, tok, width = parts.shape
    return pl.pallas_call(
        functools.partial(slopes_kernel, 1.0 / (n * tok)),
        out_shape=jax.ShapeDtypeStruct(parts.shape, bf16),
        in_specs=[VM, VM, VM],
        out_specs=VM,
        compiler_params=pltpu.CompilerParams(vmem_limit_bytes=SMALL_MIB * MIB),
        cost_estimate=pl.CostEstimate(flops=n * tok * width, bytes_accessed=4 * n * tok * width, transcendentals=0),
        name="own_slopes",
    )(parts, x, y)


def slope_kernel(z_ref, w_ref, gate_ref, up_ref, hidden_ref, s_out):
    quarter = w_ref.shape[-1]
    slope = None
    for r in range(4):
        part = contract_last(w_ref[2, r], z_ref[:, r * quarter : (r + 1) * quarter])
        slope = part if slope is None else slope + part
    slope = slope * (1.0 / math.sqrt(FF))
    gate = gate_ref[...]
    sig = jax.nn.sigmoid(gate)
    s_out[0] = (slope * up_ref[...] * (sig * (1.0 + gate * (1.0 - sig)))).astype(bf16)
    s_out[1] = (slope * (gate * sig)).astype(bf16)
    s_out[2] = hidden_ref[...]


def slope_parts(z, w, gate, up, hidden):
    rows, tokens = gate.shape
    width = z.shape[1]
    return pl.pallas_call(
        slope_kernel,
        out_shape=pltpu.VMEM((3, rows, tokens), bf16),
        in_specs=[VM] * 5,
        out_specs=VM,
        compiler_params=pltpu.CompilerParams(vmem_limit_bytes=SMALL_MIB * MIB),
        cost_estimate=pl.CostEstimate(flops=2 * rows * tokens * width, bytes_accessed=4 << 20, transcendentals=0),
        name="slope_parts",
    )(z, w, gate, up, hidden)


def adam_step(m, v, c, g, k):
    m = k[0] * m + k[1] * g
    v = k[2] * v + k[3] * (g * g)
    root = v * lax.rsqrt(v)
    c = k[4] * c - k[5] * (m / (root + epsilon))
    return m, v, c


def adam_kernel(steps, ps, r_of, lanes, pos, coef, m_ref, v_ref, w_ref, *refs):
    ins = [refs[3 * s : 3 * s + 3] for s in range(steps)]
    out_ref = refs[3 * steps]
    g_refs = refs[3 * steps + 1 :]
    i = pl.program_id(0)
    r = r_of(i)
    _, rows, quarter = g_refs[0].shape
    across = pl.ds(pl.multiple_of(r * quarter, quarter), quarter)
    for n, p in enumerate(ps):
        for s in range(steps):
            x_ref, z_ref, s_ref = ins[s]
            right = (x_ref if p < 2 else z_ref)[:, across]
            g_refs[s][n] = jnp.dot(s_ref[p], right, preferred_element_type=f32)
    step_rows = 16
    for n, p in enumerate(ps):
        ks = [[coef[12 * s + (6 if p == 2 else 0) + j] for j in range(6)] for s in range(steps)]

        @pl.loop(0, rows // step_rows, unroll=7 if (rows // step_rows) % 7 == 0 else 1)
        def _(k, n=n, p=p, ks=ks):
            at = pl.ds(pl.multiple_of(k * step_rows, step_rows), step_rows)
            for low in range(0, quarter, lanes):
                cols = slice(low, low + lanes)
                m = m_ref[0, n, at, cols].astype(f32)
                v = v_ref[0, n, at, cols].astype(f32)
                start = w_ref[p, r, at, cols].astype(f32)
                c = start
                for s in range(steps):
                    m, v, c = adam_step(m, v, c, g_refs[s][n, at, cols], ks[s])
                out_ref[n, i, at, cols] = (c if steps == 1 else start - c).astype(bf16)


def adam(pos, coef, first_moment, second_moment, w, parts, tiles):
    ps, rs = list(tiles[0]), list(tiles[1])
    steps = len(parts)
    rows, quarter = w.shape[2:]
    tokens = parts[0][0].shape[0]
    np_, nr = len(ps), len(rs)
    stride = rs[1] - rs[0] if nr > 1 else 0
    assert rs == [rs[0] + stride * k for k in range(nr)] and ps == list(range(ps[0], ps[0] + np_)) and ps[0] % np_ == 0

    def r_of(i):
        return rs[0] + stride * i

    moment = pl.BlockSpec((1, np_, rows, quarter), lambda i, pos: (0, ps[0] // np_, 0, r_of(i) ^ pos[0]))
    args = [a for part in parts for a in part]
    return pl.pallas_call(
        functools.partial(adam_kernel, steps, ps, r_of, min(512, quarter)),
        out_shape=pltpu.VMEM((np_, nr, rows, quarter), bf16),
        grid_spec=pltpu.PrefetchScalarGridSpec(
            num_scalar_prefetch=1,
            grid=(nr,),
            in_specs=[SM, moment, moment, VM] + [VM] * (3 * steps),
            out_specs=VM,
            scratch_shapes=[pltpu.VMEM((np_, rows, quarter), f32)] * steps,
        ),
        compiler_params=pltpu.CompilerParams(vmem_limit_bytes=ADAM_MIB * MIB),
        cost_estimate=pl.CostEstimate(
            flops=np_ * nr * steps * 2 * rows * tokens * quarter, bytes_accessed=np_ * nr * rows * quarter * 8, transcendentals=0
        ),
    )(pos, coef, first_moment, second_moment, w, *args)


def settle_kernel(w_ref, m_ref, own_ref, near_ref, far_ref, *refs):
    w_out, m_out = refs[-2:]
    total = own_ref[0, 0].astype(f32) + near_ref[0].astype(f32) + far_ref[...].astype(f32)
    delta = total * 0.25
    new_momentum = nesterov_coef * m_ref[0] + delta
    m_out[0] = new_momentum
    w_out[0] = w_ref[0] - outer_rate * (delta + nesterov_coef * new_momentum)


def settle(p, weights, momentum, own, near, far, before):
    _, rows, quarter = weights.shape
    half = rows // 2
    block = pl.BlockSpec((1, half, quarter), lambda i: (p, i, 0))
    shape = jax.ShapeDtypeStruct(weights.shape, f32)
    return pl.pallas_call(
        settle_kernel,
        grid=(2,),
        out_shape=[shape, shape],
        in_specs=[
            block,
            block,
            pl.BlockSpec((1, 1, half, quarter), lambda i: (p, 0, i, 0)),
            block,
            pl.BlockSpec((half, quarter), lambda i: (i, 0)),
        ]
        + [pl.BlockSpec(memory_space=pl.ANY)] * len(before),
        out_specs=[block, block],
        input_output_aliases={5 + k: k for k in range(len(before))},
        compiler_params=pltpu.CompilerParams(vmem_limit_bytes=12 * MIB),
    )(weights, momentum, own, near, far, *before)


def coefficients(skipped):
    found = []
    for s in range(2):
        for scale in (1.0 / math.sqrt(D), 1.0 / math.sqrt(FF)):
            go = (beta_first, (1.0 - beta_first) * scale, beta_second, (1.0 - beta_second) * scale * scale, 1.0 - inner_rate * decay_rate, inner_rate)
            stay = (1.0, 0.0, 1.0, 0.0, 1.0, 0.0)
            found.append(jnp.where(skipped[s], jnp.array(stay, f32), jnp.array(go, f32)))
    return jnp.concatenate(found)


def round_of(weights, momentum, first_moment, second_moment, inputs, targets, overflow_step):
    _, rows, quarter = weights.shape
    zh, co = lax.axis_index("zh"), lax.axis_index("co")
    mine = 2 * zh + co

    def own_order(array):
        parts = [lax.dynamic_slice_in_dim(array, (mine ^ r) * quarter, quarter, axis=2) for r in range(4)]
        return jnp.concatenate(parts, axis=2)

    def partner(array):
        return lax.ppermute(array, "co", [(0, 1), (1, 0)])

    def across(array):
        return lax.ppermute(array, "zh", [(0, 1), (1, 0)])

    steps, tok, width = inputs.shape
    half = width // 2
    pair = collect(inputs, "zl")
    told = jnp.max(jnp.stack([(e == jnp.arange(128, dtype=jnp.int32)).astype(bf16) for e in around(overflow_step, "zl")]), axis=0)
    own = [weights[0:2].astype(bf16), weights[2:3].astype(bf16)]
    far = []
    for chunk in own:
        far.append(across(chunk))
    near = []
    for chunk in own:
        near.append(partner(chunk))

    marks = jnp.broadcast_to(told.reshape(1, 1, 128), (2, tok, 128))
    low = jnp.concatenate([pair[:, k, :, :half] for k in range(steps)], axis=2)
    high = jnp.concatenate([pair[:, 0, :, half:], marks] + [pair[:, k, :, half:] for k in range(1, steps)], axis=2)
    flat = [m.reshape(-1, m.shape[-1]) for m in (collect(low, "y"), collect(high, "x"))]
    pieces = []
    for k in range(steps):
        start, stop = (k * half + (128 if k else 0), (k + 1) * half + 128)
        pieces.append(around(flat[0][:, k * half : (k + 1) * half], "x") + around(flat[1][:, start:stop], "y"))
    inputs, targets, far[1] = lax.optimization_barrier((inputs, targets, far[1]))
    inputs, targets = own_order(inputs), own_order(targets)
    marked = functools.reduce(jnp.maximum, [jnp.max(p[:, half : half + steps], axis=0) for p in pieces[0][4:]])
    coef = coefficients([marked[s] > 0 for s in range(steps)])
    pos = mine.reshape(1).astype(jnp.int32)
    at = jnp.stack([lax.axis_index("x"), lax.axis_index("y"), mine]).astype(jnp.int32)

    both = [partner(chunk) for chunk in far]
    w = own + near + far + both
    xs, ys = [inputs[k] for k in range(steps)], [targets[k] for k in range(steps)]
    parts = []
    w_start = None
    for k in range(steps):
        x, gate, up, hidden, sums, *w0 = forward(at, pieces[k], w, rows)
        if k == 0:
            w = w_start = w0[0]
            sums, coef, xs, ys = lax.optimization_barrier((sums, coef, xs, ys))
        arrived = lax.all_to_all(sums.reshape(-1, tok, width), FSDP, 0, 0, tiled=True)
        copies = own_slopes(arrived, xs[k], ys[k])
        z = lax.all_to_all(copies, FSDP, 0, 0, tiled=True).reshape(-1, width)
        parts.append((x, z, slope_parts(z, w, gate, up, hidden)))
        if k == 0:
            w = adam(pos, coef, first_moment, second_moment, w, parts, (range(3), range(4)))
    arrived = []
    state = (first_moment, second_moment, w_start, parts)
    for p in (2, 0, 1):
        out = adam(pos, coef, *state, ((p,), (3,)))[0, 0]
        handed = partner(out)
        kept = adam(pos, coef, *state, ((p,), (2,)))[0, 0]
        joint = (kept.astype(f32) + handed.astype(f32)).astype(bf16)
        joint, pos = lax.optimization_barrier((joint, pos))
        arrived.append((p, across(joint)))
    beside = adam(pos, coef, *state, (range(3), (1,)))
    near_part = partner(beside[:, 0])
    rest = adam(pos, coef, *state, (range(3), (0,)))
    result = ()
    for p, far_part in arrived:
        result = settle(p, weights, momentum, rest, near_part, far_part, result)
    return tuple(result)


def solution(mesh):
    grid = Mesh(mesh.devices.reshape(2, 2, 4, 2, 4), ("zh", "co", "x", "zl", "y"))
    isl, fsdp = ("zh", "co"), ("x", "zl", "y")
    in_specs = (
        P(None, fsdp, isl),
        P(None, fsdp, isl),
        P(isl, None, fsdp, None),
        P(isl, None, fsdp, None),
        P(None, isl + fsdp, None),
        P(None, isl + fsdp, None),
        P(isl, fsdp),
    )
    out_specs = (P(None, fsdp, isl), P(None, fsdp, isl))
    return jax.shard_map(round_of, mesh=grid, in_specs=in_specs, out_specs=out_specs, check_vma=False)
```
